32 devices in a mesh: fsdp: 16 (over z, y, x), tp: 2 (over core).
Axes of the slice: x: 2, y: 2, z: 4, core: 2. Of those that a mesh axis runs over, the one named last changes fastest.
Arguments:
- inputs: bfloat16 [4096, 4096], P('fsdp'), may hold values from -6 to 6
- value_grad: bfloat16 [4096, 1024], P('fsdp', 'tp'), may hold values from -24 to 24
- value_weight: bfloat16 [4096, 1024], P('tp', 'fsdp'), may hold values from -0.09375 to 0.09375
- counts: int32 [16, 4], P('fsdp'), may hold values from 1 to 232, as said below
- offsets: int32 [16, 4], P('fsdp'), may hold values from 0 to 248, as said below
Outputs:
- input_grad: bfloat16 [4096, 4096], P('fsdp', 'tp')
- weight_grad: float32 [4096, 1024], P('fsdp', 'tp')
The draws below stay inside these ranges and needn't reach their ends.
Inputs may be any that keep to these rules, and one draw needn't show every extreme that they name: `offsets`: on each index of fsdp the 4 samples lie in order; each starts at a multiple of 8, at or after the 8-row-aligned end of the previous one, and all lie within the 256 rows; on some index the aligned blocks of its samples fill all 256 rows. `counts`: how many rows the samples of a row group fill varies widely between indices of fsdp.
All inputs are finite; a program needn't handle non-finite values.
Results may differ from the reference program's by a relative error of at most 0.0046.
Values may be sent and summed in bfloat16 or wider, within the bound.
A program may use at most 64 MiB of HBM per device.

```python
import math
import jax
import jax.numpy as jnp
from jax import lax

D = 4096
KV = 1024
TOK_DEV = 256
S_DEV = 4
TOKENS = 4096
SAMPLES = 64
N_FSDP = 16


def packing_layout(key):
    units_all = TOK_DEV // 8
    spare = units_all - S_DEV
    divisor = max(spare, 1)
    first = jax.random.randint(jax.random.fold_in(key, 101), (N_FSDP,), 0, spare + 1)
    second = jax.random.randint(jax.random.fold_in(key, 102), (N_FSDP,), 0, spare + 1)
    extra = first * second // divisor
    chosen = jax.random.randint(jax.random.fold_in(key, 103), (), 0, N_FSDP)
    is_chosen = jnp.arange(N_FSDP) == chosen
    extra = jnp.where(is_chosen, spare, extra)
    raw_cuts = jax.random.randint(jax.random.fold_in(key, 104), (N_FSDP, S_DEV - 1), 0, spare + 1)
    cuts = jnp.sort(raw_cuts * extra[:, None] // divisor, axis=1)
    cuts = jnp.where(is_chosen[:, None], spare, cuts)
    edges = jnp.concatenate([jnp.zeros((N_FSDP, 1), jnp.int32), cuts.astype(jnp.int32), extra[:, None].astype(jnp.int32)], axis=1)
    units = 1 + edges[:, 1:] - edges[:, :-1]
    ends = jnp.cumsum(units, axis=1)
    offsets = (8 * (ends - units)).astype(jnp.int32)
    trims = jax.random.randint(jax.random.fold_in(key, 105), (N_FSDP, S_DEV), 0, 8)
    slots = jnp.arange(S_DEV)[None, :]
    fixed_trims = jnp.where(slots == S_DEV - 1, 7, 0)
    trims = jnp.where(is_chosen[:, None], fixed_trims, trims)
    counts = (8 * units - trims).astype(jnp.int32)
    return (counts, offsets)


def draw_counts(key, part):
    return packing_layout(key)[0]


def draw_offsets(key, part):
    return packing_layout(key)[1]


def strengthened(result, own_key, source, target, shards_of, factor):
    def block_of(dim):
        return (jnp.arange(result.shape[dim]) // (result.shape[dim] // shards_of)).reshape((-1,) + (1,) * (result.ndim - 1 - dim))

    near = jax.random.permutation(own_key, shards_of)[block_of(target)]
    second = (block_of(target) + shards_of // 2) % shards_of
    return jnp.where((block_of(source) == near) | (block_of(source) == second), factor * result, result)


def block_scale(key, extent, cuts, low, high):
    factor_of = 1.0
    for position, parts in cuts:
        heights = jax.random.uniform(jax.random.fold_in(jax.random.fold_in(key, 6), position), (parts,), jnp.float32, low / len(cuts), high / len(cuts))
        factor_of = factor_of * jnp.repeat(jnp.exp(heights), extent[position] // parts).reshape((-1,) + (1,) * (len(extent) - 1 - position))
    return factor_of


def gaussian(stream_key, shape, width, most, pieces=(), kind=jnp.bfloat16):
    level = block_scale(stream_key, shape, pieces, -0.22, 0.18) if pieces else 1.0
    entries = jax.random.normal(stream_key, shape, jnp.float32) * width * level
    return jnp.minimum(jnp.maximum(entries, -most), most).astype(kind)


def heavy_noise(stream_key, shape, deviation, limit, cuts, heavy, kind=jnp.bfloat16):
    result = deviation * jax.random.normal(stream_key, shape, jnp.float32)
    if cuts:
        result = result * block_scale(stream_key, shape, cuts, -0.22, 0.18)
    return jnp.clip(strengthened(result, jax.random.fold_in(stream_key, 3), *heavy), -limit, limit).astype(kind)


def setup_inputs(seed: int = 0) -> dict:
    keys = jax.random.split(jax.random.key(seed), 6)
    inputs = heavy_noise(keys[0], (TOKENS, D), 1.0, 6.0, ((0, 16),), (0, 1, 16, 2.0))
    value_grad = gaussian(keys[1], (TOKENS, KV), 4.0, 24.0, ((0, 16), (1, 2)))
    value_weight = gaussian(keys[2], (D, KV), D ** -0.5, 0.09375, ((0, 2), (1, 16)))
    counts = draw_counts(jax.random.fold_in(keys[5], 71), 0)
    offsets = draw_offsets(jax.random.fold_in(keys[5], 71), 0)
    return {"inputs": inputs, "value_grad": value_grad, "value_weight": value_weight, "counts": counts, "offsets": offsets}


def reference(inputs, value_grad, value_weight, counts, offsets):
    positions = jnp.arange(TOK_DEV, dtype=jnp.int32)[None, :, None]
    inside = (positions >= offsets[:, None, :]) & (positions < offsets[:, None, :] + counts[:, None, :])
    inverse_root = lax.rsqrt(counts.astype(jnp.float32))[:, None, :]
    row_factor = lax.optimization_barrier(jnp.sum(jnp.where(inside, inverse_root, jnp.zeros_like(inverse_root)), axis=2))
    scaled = (value_grad.astype(jnp.float32).reshape(N_FSDP, TOK_DEV, KV) * row_factor[:, :, None]).astype(jnp.bfloat16)

    def rows_grad(group_rows):
        return jnp.dot(group_rows, value_weight.T, preferred_element_type=jnp.float32).astype(jnp.bfloat16)
    input_grad = lax.map(rows_grad, scaled).reshape(TOKENS, D)
    weight_grad = jnp.dot(inputs.T, scaled.reshape(TOKENS, KV), preferred_element_type=jnp.float32)
    weight_grad = weight_grad * (1.0 / math.sqrt(SAMPLES))
    return (input_grad, weight_grad)
```

```python
import functools
import math

import jax
import jax.numpy as jnp
from jax import lax
from jax.experimental import pallas as pl
from jax.experimental.pallas import tpu as pltpu
from jax.sharding import PartitionSpec as P

MESH = pl.DeviceIdType.MESH
GROUP = 4
VMEM_ROOM = 48 * 2**20


def scale_rows(value_grad, counts, offsets):
    positions = jnp.arange(value_grad.shape[0], dtype=jnp.int32)[:, None]
    starts = offsets[0][None, :]
    lengths = counts[0][None, :]
    inside = (positions >= starts) & (positions < starts + lengths)
    inverse_root = lax.rsqrt(lengths.astype(jnp.float32))
    row_factor = jnp.sum(jnp.where(inside, inverse_root, jnp.zeros_like(inverse_root)), axis=1)
    return (value_grad.astype(jnp.float32) * row_factor[:, None]).astype(jnp.bfloat16)


def general(inputs, value_grad, value_weight, counts, offsets):
    tok_rows = inputs.shape[0]
    row_block = min(128, tok_rows)
    scaled = scale_rows(value_grad, counts, offsets)
    live_end = jnp.max(offsets[0] + counts[0])
    live_blocks = (live_end + row_block - 1) // row_block
    scaled_all = lax.all_gather(scaled, "tp", axis=1, tiled=True)
    empty_inputs = jnp.zeros((tok_rows, value_weight.shape[0]), jnp.float32)
    piece = lax.all_gather(value_weight, "fsdp", axis=1, tiled=True)

    def add_add_block(block_index, partial_value):
        lower = lax.dynamic_slice_in_dim(scaled_all, block_index * row_block, row_block, 0)
        before = lax.dynamic_slice_in_dim(partial_value, block_index * row_block, row_block, 0)
        product = lax.dot_general(
            lower, piece, (((1,), (1,)), ((), ())), preferred_element_type=jnp.float32
        )
        return lax.dynamic_update_slice_in_dim(
            partial_value, before + product, block_index * row_block, 0
        )

    result = lax.fori_loop(0, live_blocks, add_add_block, empty_inputs)
    input_grad = result.astype(jnp.bfloat16)
    normalizer = 1.0 / math.sqrt(counts.shape[1] * lax.axis_size("fsdp"))
    empty = jnp.zeros((inputs.shape[1], scaled.shape[1]), jnp.float32)

    def weight_add_block(block_index, partial_value):
        feature_rows = lax.dynamic_slice_in_dim(inputs, block_index * row_block, row_block, 0)
        grad_rows = lax.dynamic_slice_in_dim(scaled, block_index * row_block, row_block, 0)
        return partial_value + lax.dot_general(
            feature_rows, grad_rows, (((0,), (0,)), ((), ())), preferred_element_type=jnp.float32
        )

    result = lax.fori_loop(0, live_blocks, weight_add_block, empty)
    summed = lax.psum_scatter(result, "fsdp", scatter_dimension=0, tiled=True)
    return (input_grad, summed * normalizer)


def kernel(
    n, normalizer, x_ref, s_ref, wt_ref, dx_ref, dw_ref,
    s_own, s_sib, x_all, w_all, part_out, part_in, dx_out, dx_in,
    w_send, w_recv, s_send, s_recv, c_send, c_recv, x_send, x_recv,
    g_send, g_recv, p_send, p_recv, o_send, o_recv,
):
    nz = n // GROUP
    me = lax.axis_index("fsdp")
    core = lax.axis_index("tp")
    sib = 1 - core
    z = me // GROUP
    quarter = me % GROUP
    dx = 1 - 2 * (me % 2)
    dy = 2 - 4 * ((me // 2) % 2)
    steps = (0, dx, dy, dx + dy)
    tok = s_ref.shape[0]
    half = s_ref.shape[1]
    wcols = wt_ref.shape[0]
    fq = w_all.shape[1]
    zrows = GROUP * wcols
    hr = x_all.shape[2]
    order = [k for k in range(nz // 2, nz)] + [k for k in range(1, nz // 2)] + [0]

    def remote(src, dst, send, recv, dev):
        return pltpu.make_async_remote_copy(
            src_ref=src, dst_ref=dst, send_sem=send, recv_sem=recv,
            device_id=dev, device_id_type=MESH,
        )

    barrier = pltpu.get_barrier_semaphore()
    targets = [(me + steps[j], core) for j in range(1, GROUP)] + [(me, sib)]
    for k in range(1, nz):
        other = ((z + k) % nz) * GROUP + quarter
        targets += [(other, core), (other, sib)]
    for dev in targets:
        pl.semaphore_signal(barrier, inc=1, device_id=dev, device_id_type=MESH)
    pl.semaphore_wait(barrier, len(targets))

    def w_rows(f):
        return pl.ds(pl.multiple_of(f * wcols, wcols), wcols)

    def lanes(start, size):
        return pl.ds(pl.multiple_of(start, 128), size)

    def slot(j):
        return pl.ds(j * tok, tok)

    w_copies, s_copies, x_copies = {}, {}, {}
    for j in range(1, GROUP):
        w_copies[j] = remote(
            wt_ref.at[:, lanes((quarter + steps[j]) * fq, fq)], w_all.at[w_rows(me), :],
            w_send.at[j], w_recv.at[j], (me + steps[j], core))
        w_copies[j].start()
    own_copy = remote(s_ref, s_sib.at[slot(0), :], c_send.at[0], c_recv.at[0], (me, sib))
    own_copy.start()
    for j in (3, 1, 2):
        s_copies[j] = remote(
            s_ref, s_own.at[slot(j), :], s_send.at[j], s_recv.at[j], (me + steps[j], core))
        s_copies[j].start()

    def x_lanes(k, q):
        zk = (z + k) % nz
        return lanes(((zk * GROUP + q) * 2 + core) * hr, hr)

    for k in order:
        for j in (3, 1, 2):
            x_copies[k, j] = remote(
                x_ref.at[:, x_lanes(k, quarter + steps[j])], x_all.at[k, slot(j), :],
                x_send.at[k, j], x_recv.at[k, j], (me + steps[j], core))
            x_copies[k, j].start()
    w_all[w_rows(me), :] = wt_ref[:, lanes(quarter * fq, fq)]
    s_own[slot(0), :] = s_ref[...]
    for k in range(nz):
        x_all[k, slot(0), :] = x_ref[:, x_lanes(k, quarter)]

    def chain(origin, way, k):
        rows = pl.ds(pl.multiple_of(origin * zrows, zrows), zrows)
        dev = (me + GROUP * way, core)
        return remote(w_all.at[rows, :], w_all.at[rows, :],
                      g_send.at[(1 - way) // 2, k], g_recv.at[origin], dev)

    def chain_step(k):
        for way in (1, -1):
            origin = z - way * k
            here = (origin >= 0) & (origin < nz)
            onward = here & (z + way >= 0) & (z + way < nz)
            if k > 0:
                @pl.when(here)
                def _():
                    chain(origin, -way, k).wait_recv()

            @pl.when(onward)
            def _():
                chain(origin, way, k).start()

    for j in range(1, GROUP):
        w_copies[j].wait_recv()
    chain_step(0)

    core_copies = [own_copy]
    for j in (1, 2, 3):
        s_copies[j].wait_recv()
        copy = remote(s_own.at[slot(j), :], s_sib.at[slot(j), :], c_send.at[j], c_recv.at[j], (me, sib))
        copy.start()
        core_copies.append(copy)
    if nz > 1:
        chain_step(1)
    for copy in core_copies:
        copy.wait_recv()

    p_copies = []
    own_part = None
    next_step = 2
    for k in order:
        for j in range(1, GROUP):
            x_copies[k, j].wait_recv()
        feature_rows = x_all[k]
        dims = (((0,), (0,)), ((), ()))
        for side, grads, dst_core in ((0, s_own, core), (1, s_sib, sib)):
            part = lax.dot_general(feature_rows, grads[...], dims, preferred_element_type=jnp.float32)
            if k == 0 and side == 0:
                own_part = part
                dw_ref[pl.ds(pl.multiple_of(core * hr, hr), hr), :] = part
                continue
            part_out[k, side] = part.astype(jnp.bfloat16)
            dev = (((z + k) % nz) * GROUP + quarter, dst_core)
            copy = remote(part_out.at[k, side], part_in.at[k, side], p_send.at[k, side], p_recv.at[k, side], dev)
            copy.start()
            p_copies.append(copy)
        if next_step < nz:
            chain_step(next_step)
            next_step += 1

    o_copies = {}
    own_rows = pl.ds(pl.multiple_of(core * half, half), half)
    sib_rows = pl.ds(pl.multiple_of(sib * half, half), half)
    for j in (3, 1, 2, 0):
        product = jnp.dot(s_own[slot(j), :], w_all[own_rows, :], preferred_element_type=jnp.float32)
        product += jnp.dot(s_sib[slot(j), :], w_all[sib_rows, :], preferred_element_type=jnp.float32)
        if j == 0:
            dx_ref[:, lanes(quarter * fq, fq)] = product.astype(jnp.bfloat16)
        else:
            dx_out[j] = product.astype(jnp.bfloat16)
            o_copies[j] = remote(dx_out.at[j], dx_in.at[j], o_send.at[j], o_recv.at[j], (me + steps[j], core))
            o_copies[j].start()

    for copy in p_copies:
        copy.wait_recv()
    own_half = pl.ds(pl.multiple_of(core * hr, hr), hr)
    sib_half = pl.ds(pl.multiple_of(sib * hr, hr), hr)
    total = dw_ref[own_half, :]
    for k in range(1, nz):
        total += part_in[k, 0].astype(jnp.float32)
    dw_ref[own_half, :] = total * normalizer
    total = part_in[0, 1].astype(jnp.float32)
    for k in range(1, nz):
        total += part_in[k, 1].astype(jnp.float32)
    dw_ref[sib_half, :] = total * normalizer

    for j in (1, 2, 3):
        o_copies[j].wait_recv()
        dx_ref[:, lanes((quarter + steps[j]) * fq, fq)] = dx_in[j]

    for group in (w_copies, s_copies, x_copies, o_copies):
        for copy in group.values():
            copy.wait_send()
    for copy in core_copies + p_copies:
        copy.wait_send()
    for k in range(nz):
        for way in (1, -1):
            origin = z - way * k

            @pl.when((origin >= 0) & (origin < nz) & (z + way >= 0) & (z + way < nz))
            def _():
                chain(origin, way, k).wait_send()


def fused(n, inputs, value_grad, value_weight, counts, offsets):
    tok, width = inputs.shape
    half = value_grad.shape[1]
    wfeat, wcols = value_weight.shape
    nz = n // GROUP
    fq = wfeat // GROUP
    hr = width // n // 2
    bf, dma = jnp.bfloat16, pltpu.SemaphoreType.DMA
    normalizer = 1.0 / math.sqrt(counts.shape[1] * n)
    scaled = scale_rows(value_grad, counts, offsets)
    vmem = pl.BlockSpec(memory_space=pltpu.VMEM)
    return pl.pallas_call(
        functools.partial(kernel, n, normalizer),
        out_shape=(
            jax.ShapeDtypeStruct((tok, wfeat), bf),
            jax.ShapeDtypeStruct((2 * hr, half), jnp.float32),
        ),
        in_specs=[vmem] * 3,
        out_specs=(vmem, vmem),
        scratch_shapes=[
            pltpu.VMEM((GROUP * tok, half), bf),
            pltpu.VMEM((GROUP * tok, half), bf),
            pltpu.VMEM((nz, GROUP * tok, hr), bf),
            pltpu.VMEM((n * wcols, fq), bf),
            pltpu.VMEM((nz, 2, hr, half), bf),
            pltpu.VMEM((nz, 2, hr, half), bf),
            pltpu.VMEM((GROUP, tok, fq), bf),
            pltpu.VMEM((GROUP, tok, fq), bf),
            dma((GROUP,)), dma((GROUP,)),
            dma((GROUP,)), dma((GROUP,)),
            dma((GROUP,)), dma((GROUP,)),
            dma((nz, GROUP)), dma((nz, GROUP)),
            dma((2, nz)), dma((nz,)),
            dma((nz, 2)), dma((nz, 2)),
            dma((GROUP,)), dma((GROUP,)),
        ],
        compiler_params=pltpu.CompilerParams(
            collective_id=0, has_side_effects=True, vmem_limit_bytes=VMEM_ROOM
        ),
    )(inputs, scaled, value_weight.T)


def solution(mesh):
    n, tp = mesh.shape["fsdp"], mesh.shape["tp"]

    def local(inputs, value_grad, value_weight, counts, offsets):
        hr = inputs.shape[1] // n // 2
        fits = tp == 2 and n % GROUP == 0 and n > GROUP and hr % 128 == 0
        fits = fits and value_weight.shape[1] % 16 == 0
        if fits:
            return fused(n, inputs, value_grad, value_weight, counts, offsets)
        return general(inputs, value_grad, value_weight, counts, offsets)

    in_specs = (P("fsdp", None), P("fsdp", "tp"), P("tp", "fsdp"), P("fsdp", None), P("fsdp", None))
    out_specs = (P("fsdp", "tp"), P("fsdp", "tp"))
    return jax.shard_map(local, mesh=mesh, in_specs=in_specs, out_specs=out_specs, check_vma=False)
```

```python
import functools
import math

import jax
import jax.numpy as jnp
from jax import lax
from jax.experimental import pallas as pl
from jax.experimental.pallas import tpu as pltpu
from jax.sharding import PartitionSpec as P

MESH = pl.DeviceIdType.MESH
GROUP = 4
VMEM_ROOM = 48 * 2**20


def scale_rows(value_grad, counts, offsets):
    positions = jnp.arange(value_grad.shape[0], dtype=jnp.int32)[:, None]
    starts = offsets[0][None, :]
    lengths = counts[0][None, :]
    inside = (positions >= starts) & (positions < starts + lengths)
    inverse_root = lax.rsqrt(lengths.astype(jnp.float32))
    row_factor = jnp.sum(jnp.where(inside, inverse_root, jnp.zeros_like(inverse_root)), axis=1)
    return (value_grad.astype(jnp.float32) * row_factor[:, None]).astype(jnp.bfloat16)


def general(inputs, value_grad, value_weight, counts, offsets):
    tok_rows = inputs.shape[0]
    row_block = min(128, tok_rows)
    scaled = scale_rows(value_grad, counts, offsets)
    live_end = jnp.max(offsets[0] + counts[0])
    live_blocks = (live_end + row_block - 1) // row_block
    scaled_all = lax.all_gather(scaled, "tp", axis=1, tiled=True)
    empty_inputs = jnp.zeros((tok_rows, value_weight.shape[0]), jnp.float32)
    piece = lax.all_gather(value_weight, "fsdp", axis=1, tiled=True)

    def add_add_block(block_index, partial_value):
        lower = lax.dynamic_slice_in_dim(scaled_all, block_index * row_block, row_block, 0)
        before = lax.dynamic_slice_in_dim(partial_value, block_index * row_block, row_block, 0)
        product = lax.dot_general(
            lower, piece, (((1,), (1,)), ((), ())), preferred_element_type=jnp.float32
        )
        return lax.dynamic_update_slice_in_dim(
            partial_value, before + product, block_index * row_block, 0
        )

    result = lax.fori_loop(0, live_blocks, add_add_block, empty_inputs)
    input_grad = result.astype(jnp.bfloat16)
    normalizer = 1.0 / math.sqrt(counts.shape[1] * lax.axis_size("fsdp"))
    empty = jnp.zeros((inputs.shape[1], scaled.shape[1]), jnp.float32)

    def weight_add_block(block_index, partial_value):
        feature_rows = lax.dynamic_slice_in_dim(inputs, block_index * row_block, row_block, 0)
        grad_rows = lax.dynamic_slice_in_dim(scaled, block_index * row_block, row_block, 0)
        return partial_value + lax.dot_general(
            feature_rows, grad_rows, (((0,), (0,)), ((), ())), preferred_element_type=jnp.float32
        )

    result = lax.fori_loop(0, live_blocks, weight_add_block, empty)
    summed = lax.psum_scatter(result, "fsdp", scatter_dimension=0, tiled=True)
    return (input_grad, summed * normalizer)


def kernel(
    n, normalizer, counts_ref, offsets_ref, x_hbm, g_hbm, wt_hbm, dx_ref, dw_ref,
    x_ref, g_ref, wt_ref, s_ref, s_own, s_sib, x_all, w_all, part_own, part_out, part_in,
    swap_out, swap_in, dx_out, dx_in,
    local_sem, w_send, w_recv, s_send, s_recv, c_send, c_recv, x_send, x_recv,
    g_send, g_recv, p_send, p_recv, o_send, o_recv, swap_send, swap_recv,
):
    nz = n // GROUP
    me = lax.axis_index("fsdp")
    core = lax.axis_index("tp")
    sib = 1 - core
    z = me // GROUP
    quarter = me % GROUP
    dx = 1 - 2 * (me % 2)
    dy = 2 - 4 * ((me // 2) % 2)
    steps = (0, dx, dy, dx + dy)
    tok, half = s_ref.shape
    wcols = wt_ref.shape[0]
    fq = w_all.shape[1]
    zrows = GROUP * wcols
    hr = x_all.shape[2]
    upper = (2 * z) // nz
    order = [a + upper * (nz - 1 - 2 * a) for a in
             list(range(nz - 1, nz // 2 - 1, -1)) + list(range(nz // 2))]

    fetch_g = pltpu.make_async_copy(g_hbm, g_ref, local_sem.at[0])
    fetch_w = pltpu.make_async_copy(wt_hbm, wt_ref, local_sem.at[1])
    fetch_x = pltpu.make_async_copy(x_hbm, x_ref, local_sem.at[2])
    for fetch in (fetch_g, fetch_w, fetch_x):
        fetch.start()

    def remote(src, dst, send, recv, dev):
        return pltpu.make_async_remote_copy(
            src_ref=src, dst_ref=dst, send_sem=send, recv_sem=recv,
            device_id=dev, device_id_type=MESH,
        )

    barrier = pltpu.get_barrier_semaphore()
    for j in range(1, GROUP):
        pl.semaphore_signal(barrier, inc=1, device_id=(me + steps[j], core), device_id_type=MESH)
    pl.semaphore_signal(barrier, inc=1, device_id=(me, sib), device_id_type=MESH)
    ways = ((0, 1, z < nz - 1, z > 0), (1, -1, z > 0, z < nz - 1))
    for side, way, onward, behind in ways:
        @pl.when(onward)
        def _():
            pl.semaphore_signal(barrier, inc=1, device_id=(me + GROUP * way, core), device_id_type=MESH)

    fetch_g.wait()
    positions = lax.broadcasted_iota(jnp.int32, (tok, 128), 0)
    factor = jnp.zeros((tok, 128), jnp.float32)
    for i in range(counts_ref.shape[1]):
        start = jnp.full((tok, 128), offsets_ref[0, i], jnp.int32)
        length = jnp.full((tok, 128), counts_ref[0, i], jnp.int32)
        inside = (positions >= start) & (positions < start + length)
        factor += jnp.where(inside, lax.rsqrt(length.astype(jnp.float32)), 0.0)
    for i in range(half // 128):
        cols = slice(i * 128, (i + 1) * 128)
        scaled = (g_ref[:, cols].astype(jnp.float32) * factor).astype(jnp.bfloat16)
        s_ref[:, cols] = scaled
        s_own[0:tok, cols] = scaled
    fetch_w.wait()

    inner = (z > 0) & (z < nz - 1)

    @pl.when(inner)
    def _():
        pl.semaphore_wait(barrier, GROUP + 2)

    @pl.when(jnp.logical_not(inner))
    def _():
        pl.semaphore_wait(barrier, GROUP + 1)

    def w_rows(f):
        return pl.ds(pl.multiple_of(f * wcols, wcols), wcols)

    def lanes(start, size):
        return pl.ds(pl.multiple_of(start, 128), size)

    def slot(j):
        return pl.ds(j * tok, tok)

    w_copies, s_copies, x_copies = {}, {}, {}
    for j in (3, 1, 2):
        w_copies[j] = remote(
            wt_ref.at[:, lanes((quarter + steps[j]) * fq, fq)], w_all.at[w_rows(me), :],
            w_send.at[j], w_recv.at[j], (me + steps[j], core))
        w_copies[j].start()
    for j in (1, 2):
        s_copies[j] = remote(
            s_ref, s_own.at[slot(j), :], s_send.at[j], s_recv.at[j], (me + steps[j], core))
        s_copies[j].start()
    core_copies = [remote(s_ref, s_sib.at[slot(0), :], c_send.at[0], c_recv.at[0], (me, sib))]
    core_copies[0].start()
    fetch_x.wait()

    def x_lanes(i, q):
        return lanes(((order[i] * GROUP + q) * 2 + core) * hr, hr)

    def x_start(i):
        for j in (3, 1, 2):
            x_copies[i, j] = remote(
                x_ref.at[:, x_lanes(i, quarter + steps[j])], x_all.at[i, slot(j), :],
                x_send.at[i, j], x_recv.at[i, j], (me + steps[j], core))
            x_copies[i, j].start()

    x_start(0)
    w_all[w_rows(me), :] = wt_ref[:, lanes(quarter * fq, fq)]
    for i in range(nz):
        x_all[i, slot(0), :] = x_ref[:, x_lanes(i, quarter)]

    def chain(origin, way, k, h):
        rows = pl.ds(pl.multiple_of(origin * zrows + h * (zrows // 2), zrows // 2), zrows // 2)
        dev = (me + GROUP * way, core)
        return remote(w_all.at[rows, :], w_all.at[rows, :],
                      g_send.at[(1 - way) // 2, k, h], g_recv.at[origin, h], dev)

    def chain_step(k):
        for h in range(2):
            for side, way, onward, behind in ways:
                origin = z - way * k
                here = (origin >= 0) & (origin < nz)
                if k > 0:
                    @pl.when(here)
                    def _():
                        chain(origin, -way, k, h).wait_recv()

                @pl.when(here & onward)
                def _():
                    chain(origin, way, k, h).start()

    for j in range(1, GROUP):
        w_copies[j].wait_recv()
    chain_step(0)

    def to_core(j):
        copy = remote(s_own.at[slot(j), :], s_sib.at[slot(j), :], c_send.at[j], c_recv.at[j], (me, sib))
        copy.start()
        core_copies.append(copy)

    relays = []
    for j, onto in ((1, 2), (2, 1)):
        s_copies[j].wait_recv()
        first = (j - 1) * (tok // 2)
        copy = remote(
            s_own.at[pl.ds(j * tok + first, tok // 2), :],
            s_own.at[pl.ds(3 * tok + first, tok // 2), :],
            s_send.at[2 + j], s_recv.at[2 + j], (me + steps[onto], core))
        copy.start()
        relays.append(copy)
    for i in range(1, nz):
        x_start(i)
    for j in (1, 2):
        to_core(j)
    chain_step(1)
    for copy in relays:
        copy.wait_recv()
    to_core(3)
    for copy in core_copies:
        copy.wait_recv()

    def partial_copy(t, side, lane, way):
        return remote(part_out.at[t, lane], part_in.at[side, t, lane],
                      p_send.at[t, lane], p_recv.at[side, t, lane], (me + GROUP * way, core))

    def toward(t, side):
        return t > z if side == 0 else t < z

    def block(i):
        t = order[i]
        for j in range(1, GROUP):
            x_copies[i, j].wait_recv()
        feature_rows = x_all[i]
        dims = (((0,), (0,)), ((), ()))
        for lane, grads in ((1, s_sib), (0, s_own)):
            part = lax.dot_general(feature_rows, grads[...], dims, preferred_element_type=jnp.float32)
            part_own[t, lane] = part
            for side, way, onward, behind in ways:
                @pl.when(toward(t, side) & jnp.logical_not(behind))
                def _():
                    part_out[t, lane] = part_own[t, lane].astype(jnp.bfloat16)
                    partial_copy(t, side, lane, way).start()

    def forward(i):
        t = order[i]
        for lane in (1, 0):
            for side, way, onward, behind in ways:
                @pl.when(toward(t, side) & behind)
                def _():
                    copy = partial_copy(t, side, lane, way)
                    copy.wait_recv()
                    part_out[t, lane] = (
                        part_own[t, lane] + part_in[side, t, lane].astype(jnp.float32)
                    ).astype(jnp.bfloat16)
                    copy.start()

    block(0)
    for k in range(2, nz):
        chain_step(k)
        if k == 2:
            block(1)

    o_copies = {}
    own_rows = pl.ds(pl.multiple_of(core * half, half), half)
    sib_rows = pl.ds(pl.multiple_of(sib * half, half), half)
    for j in (3, 1, 2, 0):
        product = jnp.dot(s_own[slot(j), :], w_all[own_rows, :], preferred_element_type=jnp.float32)
        product += jnp.dot(s_sib[slot(j), :], w_all[sib_rows, :], preferred_element_type=jnp.float32)
        if j == 0:
            dx_ref[:, lanes(quarter * fq, fq)] = product.astype(jnp.bfloat16)
        else:
            dx_out[j] = product.astype(jnp.bfloat16)
            o_copies[j] = remote(dx_out.at[j], dx_in.at[j], o_send.at[j], o_recv.at[j], (me + steps[j], core))
            o_copies[j].start()

    started = 2 if nz > 2 else 1
    for i in range(nz - started):
        block(i + started)
        forward(i)
    for i in range(nz - started, nz):
        forward(i)

    swap = remote(swap_out, swap_in, swap_send, swap_recv, (me, sib))
    mine = pl.ds(pl.multiple_of(core * hr, hr), hr)
    for lane in (1, 0):
        for side, way, onward, behind in ways:
            @pl.when(behind)
            def _():
                partial_copy(z, side, lane, -way).wait_recv()
                part_own[z, lane] = part_own[z, lane] + part_in[side, z, lane].astype(jnp.float32)
        total = part_own[z, lane] * normalizer
        if lane == 1:
            swap_out[...] = total
            swap.start()
        else:
            dw_ref[mine, :] = total

    for j in (1, 2, 3):
        o_copies[j].wait_recv()
        dx_ref[:, lanes((quarter + steps[j]) * fq, fq)] = dx_in[j]
    swap.wait_recv()
    dw_ref[pl.ds(pl.multiple_of(sib * hr, hr), hr), :] = swap_in[...]

    for group in (w_copies, s_copies, x_copies, o_copies):
        for copy in group.values():
            copy.wait_send()
    for copy in core_copies + relays + [swap]:
        copy.wait_send()
    for t in range(nz):
        for lane in range(2):
            for side, way, onward, behind in ways:
                @pl.when(toward(t, side))
                def _():
                    partial_copy(t, side, lane, way).wait_send()
    for k in range(nz):
        for h in range(2):
            for side, way, onward, behind in ways:
                origin = z - way * k

                @pl.when((origin >= 0) & (origin < nz) & onward)
                def _():
                    chain(origin, way, k, h).wait_send()


def fused(n, inputs, value_grad, value_weight, counts, offsets):
    tok, width = inputs.shape
    half = value_grad.shape[1]
    wfeat, wcols = value_weight.shape
    nz = n // GROUP
    fq = wfeat // GROUP
    hr = width // n // 2
    bf, f32, dma = jnp.bfloat16, jnp.float32, pltpu.SemaphoreType.DMA
    normalizer = 1.0 / math.sqrt(counts.shape[1] * n)
    vmem = pl.BlockSpec(memory_space=pltpu.VMEM)
    smem = pl.BlockSpec(memory_space=pltpu.SMEM)
    hbm = pl.BlockSpec(memory_space=pltpu.HBM)
    return pl.pallas_call(
        functools.partial(kernel, n, normalizer),
        out_shape=(
            jax.ShapeDtypeStruct((tok, wfeat), bf),
            jax.ShapeDtypeStruct((2 * hr, half), f32),
        ),
        in_specs=[smem] * 2 + [hbm] * 3,
        out_specs=(vmem, vmem),
        scratch_shapes=[
            pltpu.VMEM((tok, width), bf),
            pltpu.VMEM((tok, half), bf),
            pltpu.VMEM((wcols, wfeat), bf),
            pltpu.VMEM((tok, half), bf),
            pltpu.VMEM((GROUP * tok, half), bf),
            pltpu.VMEM((GROUP * tok, half), bf),
            pltpu.VMEM((nz, GROUP * tok, hr), bf),
            pltpu.VMEM((n * wcols, fq), bf),
            pltpu.VMEM((nz, 2, hr, half), f32),
            pltpu.VMEM((nz, 2, hr, half), bf),
            pltpu.VMEM((2, nz, 2, hr, half), bf),
            pltpu.VMEM((hr, half), f32),
            pltpu.VMEM((hr, half), f32),
            pltpu.VMEM((GROUP, tok, fq), bf),
            pltpu.VMEM((GROUP, tok, fq), bf),
            dma((3,)),
            dma((GROUP,)), dma((GROUP,)),
            dma((GROUP + 1,)), dma((GROUP + 1,)),
            dma((GROUP,)), dma((GROUP,)),
            dma((nz, GROUP)), dma((nz, GROUP)),
            dma((2, nz, 2)), dma((nz, 2)),
            dma((nz, 2)), dma((2, nz, 2)),
            dma((GROUP,)), dma((GROUP,)),
            dma, dma,
        ],
        compiler_params=pltpu.CompilerParams(
            collective_id=0, has_side_effects=True, vmem_limit_bytes=VMEM_ROOM
        ),
    )(counts, offsets, inputs, value_grad, value_weight.T)


def solution(mesh):
    n, tp = mesh.shape["fsdp"], mesh.shape["tp"]

    def local(inputs, value_grad, value_weight, counts, offsets):
        hr = inputs.shape[1] // n // 2
        fits = tp == 2 and n % GROUP == 0 and n > GROUP and hr % 128 == 0
        fits = fits and value_weight.shape[1] % 16 == 0
        if fits:
            return fused(n, inputs, value_grad, value_weight, counts, offsets)
        return general(inputs, value_grad, value_weight, counts, offsets)

    in_specs = (P("fsdp", None), P("fsdp", "tp"), P("tp", "fsdp"), P("fsdp", None), P("fsdp", None))
    out_specs = (P("fsdp", "tp"), P("fsdp", "tp"))
    return jax.shard_map(local, mesh=mesh, in_specs=in_specs, out_specs=out_specs, check_vma=False)
```

```python
import functools
import math

import jax
import jax.numpy as jnp
from jax import lax
from jax.experimental import pallas as pl
from jax.experimental.pallas import tpu as pltpu
from jax.sharding import PartitionSpec as P

MESH = pl.DeviceIdType.MESH
GROUP = 4
VMEM_ROOM = 58 * 2**20


def scale_rows(value_grad, counts, offsets):
    positions = jnp.arange(value_grad.shape[0], dtype=jnp.int32)[:, None]
    starts = offsets[0][None, :]
    lengths = counts[0][None, :]
    inside = (positions >= starts) & (positions < starts + lengths)
    inverse_root = lax.rsqrt(lengths.astype(jnp.float32))
    row_factor = jnp.sum(jnp.where(inside, inverse_root, jnp.zeros_like(inverse_root)), axis=1)
    return (value_grad.astype(jnp.float32) * row_factor[:, None]).astype(jnp.bfloat16)


def general(inputs, value_grad, value_weight, counts, offsets):
    tok_rows = inputs.shape[0]
    row_block = min(128, tok_rows)
    scaled = scale_rows(value_grad, counts, offsets)
    live_end = jnp.max(offsets[0] + counts[0])
    live_blocks = (live_end + row_block - 1) // row_block
    scaled_all = lax.all_gather(scaled, "tp", axis=1, tiled=True)
    empty_inputs = jnp.zeros((tok_rows, value_weight.shape[0]), jnp.float32)
    piece = lax.all_gather(value_weight, "fsdp", axis=1, tiled=True)

    def add_add_block(block_index, partial_value):
        lower = lax.dynamic_slice_in_dim(scaled_all, block_index * row_block, row_block, 0)
        before = lax.dynamic_slice_in_dim(partial_value, block_index * row_block, row_block, 0)
        product = lax.dot_general(
            lower, piece, (((1,), (1,)), ((), ())), preferred_element_type=jnp.float32
        )
        return lax.dynamic_update_slice_in_dim(
            partial_value, before + product, block_index * row_block, 0
        )

    result = lax.fori_loop(0, live_blocks, add_add_block, empty_inputs)
    input_grad = result.astype(jnp.bfloat16)
    normalizer = 1.0 / math.sqrt(counts.shape[1] * lax.axis_size("fsdp"))
    empty = jnp.zeros((inputs.shape[1], scaled.shape[1]), jnp.float32)

    def weight_add_block(block_index, partial_value):
        feature_rows = lax.dynamic_slice_in_dim(inputs, block_index * row_block, row_block, 0)
        grad_rows = lax.dynamic_slice_in_dim(scaled, block_index * row_block, row_block, 0)
        return partial_value + lax.dot_general(
            feature_rows, grad_rows, (((0,), (0,)), ((), ())), preferred_element_type=jnp.float32
        )

    result = lax.fori_loop(0, live_blocks, weight_add_block, empty)
    summed = lax.psum_scatter(result, "fsdp", scatter_dimension=0, tiled=True)
    return (input_grad, summed * normalizer)


def kernel(
    n, normalizer, counts_ref, offsets_ref, x_hbm, g_hbm, wt_hbm, dx_ref, dw_ref,
    x_ref, g_ref, wt_ref, s_ref, s_own, s_sib, x_all, w_all, part_own, part_out, part_in,
    swap_out, swap_in, dx_out, dx_in,
    local_sem, w_send, w_recv, s_send, s_recv, c_send, c_recv, x_send, x_recv,
    g_send, g_recv, p_send, p_recv, o_send, o_recv, swap_send, swap_recv,
):
    nz = n // GROUP
    me = lax.axis_index("fsdp")
    core = lax.axis_index("tp")
    sib = 1 - core
    z = me // GROUP
    quarter = me % GROUP
    dx = 1 - 2 * (me % 2)
    dy = 2 - 4 * ((me // 2) % 2)
    steps = (0, dx, dy, dx + dy)
    tok, half = s_ref.shape
    wcols = wt_ref.shape[0]
    fq = w_all.shape[1]
    zrows = GROUP * wcols
    hr = x_all.shape[2]
    upper = (2 * z) // nz
    order = [a + upper * (nz - 1 - 2 * a) for a in
             list(range(nz - 1, nz // 2 - 1, -1)) + list(range(nz // 2))]

    fetch_g = pltpu.make_async_copy(g_hbm, g_ref, local_sem.at[0])
    fetch_w = pltpu.make_async_copy(wt_hbm, wt_ref, local_sem.at[1])
    fetch_x = pltpu.make_async_copy(x_hbm, x_ref, local_sem.at[2])
    for fetch in (fetch_g, fetch_w, fetch_x):
        fetch.start()

    def remote(src, dst, send, recv, dev):
        return pltpu.make_async_remote_copy(
            src_ref=src, dst_ref=dst, send_sem=send, recv_sem=recv,
            device_id=dev, device_id_type=MESH,
        )

    barrier = pltpu.get_barrier_semaphore()
    for j in range(1, GROUP):
        pl.semaphore_signal(barrier, inc=1, device_id=(me + steps[j], core), device_id_type=MESH)
    pl.semaphore_signal(barrier, inc=1, device_id=(me, sib), device_id_type=MESH)
    ways = ((0, 1, z < nz - 1, z > 0), (1, -1, z > 0, z < nz - 1))
    for side, way, onward, behind in ways:
        @pl.when(onward)
        def _():
            pl.semaphore_signal(barrier, inc=1, device_id=(me + GROUP * way, core), device_id_type=MESH)

    fetch_g.wait()
    positions = lax.broadcasted_iota(jnp.int32, (tok, 128), 0)
    factor = jnp.zeros((tok, 128), jnp.float32)
    for i in range(counts_ref.shape[1]):
        start = jnp.full((tok, 128), offsets_ref[0, i], jnp.int32)
        length = jnp.full((tok, 128), counts_ref[0, i], jnp.int32)
        inside = (positions >= start) & (positions < start + length)
        factor += jnp.where(inside, lax.rsqrt(length.astype(jnp.float32)), 0.0)
    for i in range(half // 128):
        cols = slice(i * 128, (i + 1) * 128)
        scaled = (g_ref[:, cols].astype(jnp.float32) * factor).astype(jnp.bfloat16)
        s_ref[:, cols] = scaled
        s_own[0:tok, cols] = scaled
    fetch_w.wait()

    inner = (z > 0) & (z < nz - 1)

    @pl.when(inner)
    def _():
        pl.semaphore_wait(barrier, GROUP + 2)

    @pl.when(jnp.logical_not(inner))
    def _():
        pl.semaphore_wait(barrier, GROUP + 1)

    def w_rows(f):
        return pl.ds(pl.multiple_of(f * wcols, wcols), wcols)

    def lanes(start, size):
        return pl.ds(pl.multiple_of(start, 128), size)

    def slot(j):
        return pl.ds(j * tok, tok)

    w_copies, s_copies, x_copies = {}, {}, {}
    for j in (3, 1, 2):
        w_copies[j] = remote(
            wt_ref.at[:, lanes((quarter + steps[j]) * fq, fq)], w_all.at[w_rows(me), :],
            w_send.at[j], w_recv.at[j], (me + steps[j], core))
        w_copies[j].start()
    for j in (1, 2):
        s_copies[j] = remote(
            s_ref, s_own.at[slot(j), :], s_send.at[j], s_recv.at[j], (me + steps[j], core))
        s_copies[j].start()
    core_copies = [remote(s_ref, s_sib.at[slot(0), :], c_send.at[0], c_recv.at[0], (me, sib))]
    core_copies[0].start()
    fetch_x.wait()

    def x_lanes(i, q):
        return lanes(((order[i] * GROUP + q) * 2 + core) * hr, hr)

    def x_start(i):
        for j in (3, 1, 2):
            x_copies[i, j] = remote(
                x_ref.at[:, x_lanes(i, quarter + steps[j])], x_all.at[i, slot(j), :],
                x_send.at[i, j], x_recv.at[i, j], (me + steps[j], core))
            x_copies[i, j].start()

    x_start(0)
    w_all[w_rows(me), :] = wt_ref[:, lanes(quarter * fq, fq)]
    for i in range(nz):
        x_all[i, slot(0), :] = x_ref[:, x_lanes(i, quarter)]

    def chain(origin, way, k, h):
        rows = pl.ds(pl.multiple_of(origin * zrows + h * (zrows // 2), zrows // 2), zrows // 2)
        dev = (me + GROUP * way, core)
        return remote(w_all.at[rows, :], w_all.at[rows, :],
                      g_send.at[(1 - way) // 2, k, h], g_recv.at[origin, h], dev)

    def chain_step(k):
        for h in range(2):
            for side, way, onward, behind in ways:
                origin = z - way * k
                here = (origin >= 0) & (origin < nz)
                if k > 0:
                    @pl.when(here)
                    def _():
                        chain(origin, -way, k, h).wait_recv()

                @pl.when(here & onward)
                def _():
                    chain(origin, way, k, h).start()

    for j in range(1, GROUP):
        w_copies[j].wait_recv()
    chain_step(0)

    def to_core(j):
        copy = remote(s_own.at[slot(j), :], s_sib.at[slot(j), :], c_send.at[j], c_recv.at[j], (me, sib))
        copy.start()
        core_copies.append(copy)

    relays = []
    for j, onto in ((1, 2), (2, 1)):
        s_copies[j].wait_recv()
        first = (j - 1) * (tok // 2)
        copy = remote(
            s_own.at[pl.ds(j * tok + first, tok // 2), :],
            s_own.at[pl.ds(3 * tok + first, tok // 2), :],
            s_send.at[2 + j], s_recv.at[2 + j], (me + steps[onto], core))
        copy.start()
        relays.append(copy)
    for i in range(1, nz):
        x_start(i)
    for j in (1, 2):
        to_core(j)
    chain_step(1)
    for copy in relays:
        copy.wait_recv()
    to_core(3)
    for copy in core_copies:
        copy.wait_recv()

    def partial_copy(t, side, lane, way):
        return remote(part_out.at[t, lane], part_in.at[side, t, lane],
                      p_send.at[t, lane], p_recv.at[side, t, lane], (me + GROUP * way, core))

    def toward(t, side):
        return t > z if side == 0 else t < z

    def block(i):
        t = order[i]
        for j in range(1, GROUP):
            x_copies[i, j].wait_recv()
        feature_rows = x_all[i]
        dims = (((0,), (0,)), ((), ()))
        for lane, grads in ((1, s_sib), (0, s_own)):
            part = lax.dot_general(feature_rows, grads[...], dims, preferred_element_type=jnp.float32)
            part_own[t, lane] = part
            for side, way, onward, behind in ways:
                @pl.when(toward(t, side) & jnp.logical_not(behind))
                def _():
                    part_out[t, lane] = part_own[t, lane].astype(jnp.bfloat16)
                    partial_copy(t, side, lane, way).start()

    def forward(i):
        t = order[i]
        for lane in (1, 0):
            for side, way, onward, behind in ways:
                @pl.when(toward(t, side) & behind)
                def _():
                    copy = partial_copy(t, side, lane, way)
                    copy.wait_recv()
                    part_out[t, lane] = (
                        part_own[t, lane] + part_in[side, t, lane].astype(jnp.float32)
                    ).astype(jnp.bfloat16)
                    copy.start()

    block(0)
    for k in range(2, nz):
        chain_step(k)
        if k == 2:
            block(1)

    o_copies = {}
    own_rows = pl.ds(pl.multiple_of(core * half, half), half)
    sib_rows = pl.ds(pl.multiple_of(sib * half, half), half)
    for j in (3, 1, 2, 0):
        product = jnp.dot(s_own[slot(j), :], w_all[own_rows, :], preferred_element_type=jnp.float32)
        product += jnp.dot(s_sib[slot(j), :], w_all[sib_rows, :], preferred_element_type=jnp.float32)
        if j == 0:
            dx_ref[:, lanes(quarter * fq, fq)] = product.astype(jnp.bfloat16)
        else:
            dx_out[j] = product.astype(jnp.bfloat16)
            o_copies[j] = remote(dx_out.at[j], dx_in.at[j], o_send.at[j], o_recv.at[j], (me + steps[j], core))
            o_copies[j].start()

    started = 2 if nz > 2 else 1
    for i in range(nz - started):
        block(i + started)
        forward(i)
    for i in range(nz - started, nz):
        forward(i)

    swap = remote(swap_out, swap_in, swap_send, swap_recv, (me, sib))
    mine = pl.ds(pl.multiple_of(core * hr, hr), hr)
    for lane in (1, 0):
        for side, way, onward, behind in ways:
            @pl.when(behind)
            def _():
                partial_copy(z, side, lane, -way).wait_recv()
                part_own[z, lane] = part_own[z, lane] + part_in[side, z, lane].astype(jnp.float32)
        total = part_own[z, lane] * normalizer
        if lane == 1:
            swap_out[...] = total
            swap.start()
        else:
            dw_ref[mine, :] = total

    for j in (1, 2, 3):
        o_copies[j].wait_recv()
        dx_ref[:, lanes((quarter + steps[j]) * fq, fq)] = dx_in[j]
    swap.wait_recv()
    dw_ref[pl.ds(pl.multiple_of(sib * hr, hr), hr), :] = swap_in[...]

    for group in (w_copies, s_copies, x_copies, o_copies):
        for copy in group.values():
            copy.wait_send()
    for copy in core_copies + relays + [swap]:
        copy.wait_send()
    for t in range(nz):
        for lane in range(2):
            for side, way, onward, behind in ways:
                @pl.when(toward(t, side))
                def _():
                    partial_copy(t, side, lane, way).wait_send()
    for k in range(nz):
        for h in range(2):
            for side, way, onward, behind in ways:
                origin = z - way * k

                @pl.when((origin >= 0) & (origin < nz) & onward)
                def _():
                    chain(origin, way, k, h).wait_send()


def fused(n, inputs, value_grad, value_weight, counts, offsets):
    tok, width = inputs.shape
    half = value_grad.shape[1]
    wfeat, wcols = value_weight.shape
    nz = n // GROUP
    fq = wfeat // GROUP
    hr = width // n // 2
    bf, f32, dma = jnp.bfloat16, jnp.float32, pltpu.SemaphoreType.DMA
    normalizer = 1.0 / math.sqrt(counts.shape[1] * n)
    vmem = pl.BlockSpec(memory_space=pltpu.VMEM)
    smem = pl.BlockSpec(memory_space=pltpu.SMEM)
    hbm = pl.BlockSpec(memory_space=pltpu.HBM)
    return pl.pallas_call(
        functools.partial(kernel, n, normalizer),
        out_shape=(
            jax.ShapeDtypeStruct((tok, wfeat), bf),
            jax.ShapeDtypeStruct((2 * hr, half), f32),
        ),
        in_specs=[smem] * 2 + [hbm] * 3,
        out_specs=(vmem, vmem),
        scratch_shapes=[
            pltpu.VMEM((tok, width), bf),
            pltpu.VMEM((tok, half), bf),
            pltpu.VMEM((wcols, wfeat), bf),
            pltpu.VMEM((tok, half), bf),
            pltpu.VMEM((GROUP * tok, half), bf),
            pltpu.VMEM((GROUP * tok, half), bf),
            pltpu.VMEM((nz, GROUP * tok, hr), bf),
            pltpu.VMEM((n * wcols, fq), bf),
            pltpu.VMEM((nz, 2, hr, half), f32),
            pltpu.VMEM((nz, 2, hr, half), bf),
            pltpu.VMEM((2, nz, 2, hr, half), bf),
            pltpu.VMEM((hr, half), f32),
            pltpu.VMEM((hr, half), f32),
            pltpu.VMEM((GROUP, tok, fq), bf),
            pltpu.VMEM((GROUP, tok, fq), bf),
            dma((3,)),
            dma((GROUP,)), dma((GROUP,)),
            dma((GROUP + 1,)), dma((GROUP + 1,)),
            dma((GROUP,)), dma((GROUP,)),
            dma((nz, GROUP)), dma((nz, GROUP)),
            dma((2, nz, 2)), dma((nz, 2)),
            dma((nz, 2)), dma((2, nz, 2)),
            dma((GROUP,)), dma((GROUP,)),
            dma, dma,
        ],
        compiler_params=pltpu.CompilerParams(
            collective_id=0, has_side_effects=True, vmem_limit_bytes=VMEM_ROOM
        ),
    )(counts, offsets, inputs, value_grad, value_weight.T)


def solution(mesh):
    n, tp = mesh.shape["fsdp"], mesh.shape["tp"]

    def local(inputs, value_grad, value_weight, counts, offsets):
        hr = inputs.shape[1] // n // 2
        fits = tp == 2 and n % GROUP == 0 and n > GROUP and hr % 128 == 0
        fits = fits and value_weight.shape[1] % 16 == 0
        if fits:
            return fused(n, inputs, value_grad, value_weight, counts, offsets)
        return general(inputs, value_grad, value_weight, counts, offsets)

    in_specs = (P("fsdp", None), P("fsdp", "tp"), P("tp", "fsdp"), P("fsdp", None), P("fsdp", None))
    out_specs = (P("fsdp", "tp"), P("fsdp", "tp"))
    return jax.shard_map(local, mesh=mesh, in_specs=in_specs, out_specs=out_specs, check_vma=False)
```
